32 devices in a mesh: region: 16 (over z, y, x), mp: 2 (over core).
Axes of the slice: x: 2, y: 2, z: 4, core: 2. Of those that a mesh axis runs over, the one named last changes fastest.
Arguments:
- grid: bfloat16 [32768, 1024], P('region', 'mp'), may hold values from -6 to 6
- g2m_weight: float32 [32768], P('region'), may hold values from 0.3 to 1
- g2m_slot: int32 [32768], P('region'), may hold values from 0 to 511
- slot_node: int32 [16, 16, 32], P('region'), may hold values from 0 to 511, as said below
- peer_mask: int32 [16, 4], P('region'), may hold values 0 or 1
- norm_gain: float32 [1024], replicated, may hold values from 0.25 to 1.75
- w_qkv: bfloat16 [3, 1024, 1024], P(None, None, 'mp')
- w_out: bfloat16 [1024, 1024], P('mp'), may hold values from -0.1875 to 0.1875
Outputs:
- mesh_state: float32 [8192, 1024], P('region', 'mp')
- grid_out: bfloat16 [32768, 1024], P('region', 'mp')
The draws below stay inside these ranges and needn't reach their ends.
Inputs may be any that keep to these rules, and one draw needn't show every extreme that they name: `slot_node`: for each mesh tile o and lane c, the entries over all grid tiles r lie in one range b * (16) to (b + 1) * 16 - 1 and name every node of that range, where the range b depends on o and c and different lanes of one mesh tile take different ranges; so every mesh node is named by some send slot, and the 32 slots of one grid tile for one mesh tile name different nodes.
All inputs are finite; a program needn't handle non-finite values. No bound on the sum of `peer_mask` on one device may be relied on, other than what follows from the above.
Results may differ from the reference program's by a relative error of at most 0.006.
Values may be sent and summed in bfloat16 or wider, within the bound.
A program may use at most 192 MiB of HBM per device.

```python
import math
import jax
import jax.numpy as jnp
from jax import lax

D = 1024
HEADS = 16
HEAD_DIM = 64
MESH_DEV = 512
GRID_DEV = 2048
SEND_SLOTS = 512
GRID = 32768
N_REGION = 16


def draw_slot_node(key, part):
    cap = SEND_SLOTS // N_REGION
    stride = MESH_DEV // cap
    keys = jax.random.split(jax.random.fold_in(key, 17), N_REGION * cap)
    orders = jax.vmap(lambda k: jax.random.permutation(k, N_REGION))(keys).astype(jnp.int32)
    orders = orders.reshape(N_REGION, cap, N_REGION)
    lane_keys = jax.random.split(jax.random.fold_in(key, 23), N_REGION)
    ranges = jax.vmap(lambda k: jax.random.permutation(k, cap))(lane_keys).astype(jnp.int32)
    table = orders % stride + ranges[:, :, None] * stride
    return jnp.transpose(table, (0, 2, 1)).astype(jnp.int32)


def draw_w_qkv(key, part):
    first = jax.random.fold_in(jax.random.fold_in(key, 29), 0)
    base = jax.random.normal(first, (3, D, D), jnp.float32) * D ** (-0.5)
    return base.astype(jnp.bfloat16)


def place_ends(array, own_key, least, largest):
    extent = array.shape
    place = [jax.random.randint(jax.random.fold_in(own_key, axis), (), 0, extent[axis]) for axis in range(len(extent))]
    array = array.at[tuple(place)].set(least)
    longest = extent.index(max(extent))
    place[longest] = (place[longest] + 1) % extent[longest]
    return array.at[tuple(place)].set(largest)


def shard_levels(rng, shape, cuts, least, top_value):
    def one(dim, parts):
        heights = jax.random.uniform(jax.random.fold_in(jax.random.fold_in(rng, 6), dim), (parts,), jnp.float32, least / len(cuts), top_value / len(cuts))
        return jnp.repeat(jnp.exp(heights), shape[dim] // parts).reshape((-1,) + (1,) * (len(shape) - dim - 1))

    loudness = one(*cuts[0])
    for cut in cuts[1:]:
        loudness = loudness * one(*cut)
    return loudness


def centred(stream_key, extent, scale, limit, pieces=(), kind=jnp.bfloat16):
    loudness = shard_levels(stream_key, extent, pieces, -0.22, 0.18) if pieces else 1.0
    entries = jax.random.normal(stream_key, extent, jnp.float32) * scale * loudness
    return jnp.minimum(jnp.maximum(entries, -limit), limit).astype(kind)


def setup_inputs(seed: int = 0) -> dict:
    streams_of = jax.random.split(jax.random.key(seed), 9)
    return {
        "grid": centred(streams_of[0], (GRID, D), 1.0, 6.0, ((0, 16), (1, 2))),
        "g2m_weight": jnp.clip(jnp.exp(math.log(1.0) - 1.2039728 * jax.random.uniform(streams_of[1], (GRID,), jnp.float32) ** shard_levels(streams_of[1], (GRID,), ((0, 16),), -0.2, 0.2)), 0.3, 1.0),
        "g2m_slot": place_ends(jax.random.randint(streams_of[2], (GRID,), 0, SEND_SLOTS), jax.random.fold_in(streams_of[2], 1), 0, SEND_SLOTS - 1).astype(jnp.int32),
        "slot_node": draw_slot_node(jax.random.fold_in(streams_of[8], 71), 0),
        "peer_mask": place_ends((jax.random.randint(streams_of[4], (N_REGION, 4), 0, 4) < 3).astype(jnp.int32), jax.random.fold_in(streams_of[4], 1), 0, 1),
        "norm_gain": jnp.clip(1.0 + 0.15 * jax.random.normal(streams_of[5], (D,), jnp.float32), 0.25, 1.75),
        "w_qkv": draw_w_qkv(jax.random.fold_in(streams_of[8], 71), 0),
        "w_out": centred(streams_of[7], (D, D), D ** -0.5, 0.1875, ((0, 2),)),
    }


OFFSETS = (-2, -1, 1, 2)

def reference(grid, g2m_weight, g2m_slot, slot_node, peer_mask, norm_gain, w_qkv, w_out):
    regions = N_REGION
    cap = SEND_SLOTS // N_REGION
    scaled = (g2m_weight[:, None] * grid.astype(jnp.float32)).astype(jnp.bfloat16)
    scaled = scaled.reshape(regions, GRID_DEV, D)
    slot_tiles = g2m_slot.reshape(regions, GRID_DEV).astype(jnp.int32)

    def tile_partial(pair):
        values, slots = pair
        onehot = (slots[None, :] == jnp.arange(SEND_SLOTS, dtype=jnp.int32)[:, None]).astype(jnp.bfloat16)
        return jnp.dot(onehot, values, preferred_element_type=jnp.float32).astype(jnp.bfloat16)
    partial_value = lax.map(tile_partial, (scaled, slot_tiles))
    owners = jnp.arange(SEND_SLOTS, dtype=jnp.int32) // cap
    by_grid = jnp.transpose(slot_node, (1, 0, 2)).reshape(regions, SEND_SLOTS).astype(jnp.int32)
    node_table = (owners[None, :] * MESH_DEV + by_grid).astype(jnp.int32)
    mesh_in = jax.ops.segment_sum(partial_value.reshape(-1, D).astype(jnp.float32), node_table.reshape(-1), num_segments=MESH_DEV * regions)
    mesh_low = lax.optimization_barrier(mesh_in.astype(jnp.bfloat16)).astype(jnp.float32)
    normed = (mesh_low * lax.rsqrt(lax.optimization_barrier(jnp.mean(mesh_low * mesh_low, axis=-1, keepdims=True)) + 1e-05) * norm_gain).astype(jnp.bfloat16)
    queries = jnp.dot(normed, w_qkv[0], preferred_element_type=jnp.float32).astype(jnp.bfloat16)
    keys = jnp.dot(normed, w_qkv[1], preferred_element_type=jnp.float32).astype(jnp.bfloat16)
    values = jnp.dot(normed, w_qkv[2], preferred_element_type=jnp.float32).astype(jnp.bfloat16)
    q_tiles = queries.reshape(regions, MESH_DEV, HEADS, HEAD_DIM)
    k_tiles = keys.reshape(regions, MESH_DEV, HEADS, HEAD_DIM)
    v_tiles = values.reshape(regions, MESH_DEV, HEADS, HEAD_DIM)

    def tile_attend(tile):
        order = [tile] + [(tile + offset) % regions for offset in OFFSETS]
        key_block = jnp.concatenate([k_tiles[index] for index in order], axis=0)
        val_block = jnp.concatenate([v_tiles[index] for index in order], axis=0)
        active = jnp.concatenate([jnp.ones((1,), jnp.int32), peer_mask[tile].astype(jnp.int32)])
        valid = jnp.repeat(active, MESH_DEV)
        scores = jnp.einsum('qhd,khd->hqk', q_tiles[tile].astype(jnp.float32), key_block.astype(jnp.float32)) * HEAD_DIM ** (-0.5)
        scores = jnp.where(valid[None, None, :] > 0, scores, -1e+30)
        top = lax.optimization_barrier(jnp.max(scores, axis=-1, keepdims=True))
        expd = jnp.exp(scores - top)
        weights = (expd / lax.optimization_barrier(jnp.sum(expd, axis=-1, keepdims=True))).astype(jnp.bfloat16)
        out = jnp.einsum('hqk,khd->qhd', weights.astype(jnp.float32), val_block.astype(jnp.float32))
        return out.astype(jnp.bfloat16).reshape(MESH_DEV, D)
    attended = lax.map(tile_attend, jnp.arange(regions, dtype=jnp.int32)).reshape(-1, D)
    mesh_state = mesh_in + jnp.dot(attended, w_out, preferred_element_type=jnp.float32)
    mesh_back = mesh_state.astype(jnp.bfloat16)
    point_nodes = jnp.take_along_axis(node_table, slot_tiles, axis=1).reshape(-1)
    grid_out = (grid.astype(jnp.float32) + mesh_back[point_nodes].astype(jnp.float32)).astype(jnp.bfloat16)
    return (mesh_state, grid_out)
```

```python
import functools

import jax
import jax.numpy as jnp
from jax import lax
from jax.experimental import pallas as pl
from jax.experimental.pallas import tpu as pltpu
from jax.sharding import PartitionSpec as P

HEAD_DIM = 64
PAD = 80
OFFSETS = (0, -1, 1, -2, 2)
MASK_COLUMN = (1, 2, 0, 3)
MESH = pl.DeviceIdType.MESH
LOG2E = 1.4426950408889634


def exchange_kernel(n, x_ref, o_ref, send, recv, local):
    me = lax.axis_index("region")
    rows = x_ref.shape[0] // n
    barrier = pltpu.get_barrier_semaphore()

    def hello(d, carry):
        pl.semaphore_signal(
            barrier, inc=1, device_id={"region": lax.rem(me + d, n)}, device_id_type=MESH
        )
        return carry

    lax.fori_loop(1, n, hello, 0)
    mine = pl.ds(pl.multiple_of(me * rows, rows), rows)
    own = pltpu.make_async_copy(x_ref.at[mine], o_ref.at[mine], local)
    own.start()
    pl.semaphore_wait(barrier, n - 1)

    def copy(d):
        peer = lax.rem(me + d, n)
        return pltpu.make_async_remote_copy(
            src_ref=x_ref.at[pl.ds(pl.multiple_of(peer * rows, rows), rows)],
            dst_ref=o_ref.at[mine],
            send_sem=send.at[d],
            recv_sem=recv.at[d],
            device_id={"region": peer},
            device_id_type=MESH,
        )

    def begin(d, carry):
        copy(d).start()
        return carry

    def finish(d, carry):
        copy(d).wait()
        return carry

    lax.fori_loop(1, n, begin, 0)
    own.wait()
    lax.fori_loop(1, n, finish, 0)


def exchange(x, n, cid):
    return pl.pallas_call(
        functools.partial(exchange_kernel, n),
        out_shape=jax.ShapeDtypeStruct(x.shape, x.dtype),
        in_specs=[pl.BlockSpec(memory_space=pltpu.VMEM)],
        out_specs=pl.BlockSpec(memory_space=pltpu.VMEM),
        scratch_shapes=[
            pltpu.SemaphoreType.DMA((n,)),
            pltpu.SemaphoreType.DMA((n,)),
            pltpu.SemaphoreType.DMA,
        ],
        compiler_params=pltpu.CompilerParams(collective_id=cid, has_side_effects=True),
    )(x)


def layer_kernel(
    n, mp, x_ref, gain_ref, w_ref, wo_ref, mask_ref, state_ref, back_ref,
    gath, nrm, qm, kbuf, vbuf, acc, top, att, out_part, in_part,
    local, psend, precv, msend, mrecv, rsend, rrecv,
):
    region = lax.axis_index("region")
    core = lax.axis_index("mp")
    rows, width = x_ref.shape
    heads = width // HEAD_DIM
    slots = len(OFFSETS)
    barrier = pltpu.get_barrier_semaphore()
    for off in OFFSETS[1:]:
        pl.semaphore_signal(
            barrier, inc=1, device_id={"region": lax.rem(region + off + n, n)}, device_id_type=MESH
        )
    for j in range(1, mp):
        pl.semaphore_signal(
            barrier, inc=1, device_id={"mp": lax.rem(core + j, mp)}, device_id_type=MESH
        )
    own = pltpu.make_async_copy(x_ref, gath.at[0, core], local)
    own.start()
    acc[...] = jnp.zeros_like(acc)
    top[...] = jnp.full_like(top, -1e30)
    pl.semaphore_wait(barrier, slots - 1 + mp - 1)

    def to_core(s, j):
        return pltpu.make_async_remote_copy(
            src_ref=x_ref if isinstance(s, int) else gath.at[s, core],
            dst_ref=gath.at[s, core],
            send_sem=msend.at[s, j],
            recv_sem=mrecv.at[s, j],
            device_id={"mp": lax.rem(core + j, mp)},
            device_id_type=MESH,
        )

    def to_peer(s):
        mirror = (0, 2, 1, 4, 3)[s]
        return pltpu.make_async_remote_copy(
            src_ref=x_ref,
            dst_ref=gath.at[mirror, core],
            send_sem=psend.at[mirror],
            recv_sem=precv.at[mirror],
            device_id={"region": lax.rem(region + OFFSETS[s] + n, n)},
            device_id_type=MESH,
        )

    def from_peer(s):
        return pltpu.make_async_remote_copy(
            src_ref=x_ref,
            dst_ref=gath.at[s, core],
            send_sem=psend.at[s],
            recv_sem=precv.at[s],
            device_id={"region": region},
            device_id_type=MESH,
        )

    for j in range(1, mp):
        to_core(0, j).start()
    for s in range(1, slots):
        to_peer(s).start()
    own.wait()

    def relay(s):
        from_peer(s).wait_recv()
        for j in range(1, mp):
            to_core(s, j).start()

    def block(s, carry):
        for j in range(1, mp):
            to_core(s, j).wait_recv()
        square = jnp.zeros((rows, 1), jnp.float32)
        for m in range(mp):
            part = gath[s, m].astype(jnp.float32)
            square += jnp.sum(part * part, axis=-1, keepdims=True)
        inv = lax.rsqrt(square / (mp * width) + 1e-05)
        for m in range(mp):
            cols = slice(m * width, (m + 1) * width)
            nrm[:, cols] = (gath[s, m].astype(jnp.float32) * inv * gain_ref[:, cols]).astype(
                jnp.bfloat16
            )
        seen = mask_ref[s]

        @pl.when(s == 0)
        def _():
            q = jnp.dot(nrm[...], w_ref[0], preferred_element_type=jnp.float32)
            q = q * (LOG2E * HEAD_DIM ** (-0.5))
            lane = lax.broadcasted_iota(jnp.int32, (rows, 2 * HEAD_DIM), 1)
            for h in range(heads):
                pair = q[:, h // 2 * 2 * HEAD_DIM : (h // 2 + 1) * 2 * HEAD_DIM]
                keep = (lane < HEAD_DIM) if h % 2 == 0 else (lane >= HEAD_DIM)
                qm[h] = jnp.where(keep, pair, 0.0).astype(jnp.bfloat16)

        keys = jnp.dot(nrm[...], w_ref[1], preferred_element_type=jnp.float32)
        for g in range(heads // 2):
            kbuf[g] = keys[:, g * 2 * HEAD_DIM : (g + 1) * 2 * HEAD_DIM].astype(jnp.bfloat16)
        vals = jnp.dot(nrm[...], w_ref[2], preferred_element_type=jnp.float32)
        turned = vals.T * seen
        row = lax.broadcasted_iota(jnp.int32, (PAD - HEAD_DIM, rows), 0)
        extra = jnp.where(row == 0, jnp.broadcast_to(seen, row.shape), 0.0).astype(jnp.bfloat16)
        for h in range(heads):
            vbuf[h, :HEAD_DIM] = turned[h * HEAD_DIM : (h + 1) * HEAD_DIM].astype(jnp.bfloat16)
            vbuf[h, HEAD_DIM:] = extra

        @pl.when(jnp.logical_and(s >= 1, s < slots - 1))
        def _():
            relay(s + 1)

        def two_heads(g, carry):
            key = kbuf[g]
            for e in range(2):
                h = 2 * g + e
                scores = lax.dot_general(
                    key, qm[h], (((1,), (1,)), ((), ())), preferred_element_type=jnp.float32
                )
                old = top[h]
                new = jnp.maximum(old, jnp.max(scores, axis=0, keepdims=True))
                weights = jnp.exp2(scores - new).astype(jnp.bfloat16)
                scale = jnp.where(seen > 0, jnp.exp2(old - new), 1.0)
                acc[h] = acc[h] * scale + jnp.dot(
                    vbuf[h], weights, preferred_element_type=jnp.float32
                )
                top[h] = jnp.where(seen > 0, new, old)
            return carry

        lax.fori_loop(0, heads // 2, two_heads, 0)

        @pl.when(s == 0)
        def _():
            relay(s + 1)

        return carry

    lax.fori_loop(0, slots, block, 0)
    for h in range(heads):
        mix = acc[h]
        att[h * HEAD_DIM : (h + 1) * HEAD_DIM] = mix[:HEAD_DIM] / mix[HEAD_DIM : HEAD_DIM + 1]
    attended = att[...].T.astype(jnp.bfloat16)

    def product(m):
        cols = pl.ds(pl.multiple_of(m * width, width), width)
        return jnp.dot(attended, wo_ref[:, cols], preferred_element_type=jnp.float32)

    def share(j):
        return pltpu.make_async_remote_copy(
            src_ref=out_part.at[j],
            dst_ref=in_part.at[j],
            send_sem=rsend.at[j],
            recv_sem=rrecv.at[j],
            device_id={"mp": lax.rem(core + j, mp)},
            device_id_type=MESH,
        )

    for j in range(1, mp):
        out_part[j] = product(lax.rem(core + j, mp))
        share(j).start()
    total = x_ref[...].astype(jnp.float32) + product(core)
    for j in range(1, mp):
        share(j).wait()
        total += in_part[j]
    state_ref[...] = total
    back_ref[...] = total.astype(jnp.bfloat16)
    for s in range(1, slots):
        to_peer(s).wait_send()

    def drain(s, carry):
        for j in range(1, mp):
            to_core(s, j).wait_send()
        return carry

    lax.fori_loop(0, slots, drain, 0)


def layer(x, gain, w_qkv, w_out, mask, n, mp, cid):
    rows, width = x.shape
    heads = width // HEAD_DIM
    slots = len(OFFSETS)
    bf16, f32 = jnp.bfloat16, jnp.float32
    vmem = pl.BlockSpec(memory_space=pltpu.VMEM)
    dma = pltpu.SemaphoreType.DMA
    return pl.pallas_call(
        functools.partial(layer_kernel, n, mp),
        out_shape=(
            jax.ShapeDtypeStruct((rows, width), f32),
            jax.ShapeDtypeStruct((rows, width), bf16),
        ),
        in_specs=[vmem] * 5,
        out_specs=(vmem, vmem),
        scratch_shapes=[
            pltpu.VMEM((slots, mp, rows, width), bf16),
            pltpu.VMEM((rows, mp * width), bf16),
            pltpu.VMEM((heads, rows, 2 * HEAD_DIM), bf16),
            pltpu.VMEM((heads // 2, rows, 2 * HEAD_DIM), bf16),
            pltpu.VMEM((heads, PAD, rows), bf16),
            pltpu.VMEM((heads, PAD, rows), f32),
            pltpu.VMEM((heads, 1, rows), f32),
            pltpu.VMEM((width, rows), f32),
            pltpu.VMEM((mp, rows, width), f32),
            pltpu.VMEM((mp, rows, width), f32),
            dma,
            dma((slots,)),
            dma((slots,)),
            dma((slots, mp)),
            dma((slots, mp)),
            dma((mp,)),
            dma((mp,)),
        ],
        compiler_params=pltpu.CompilerParams(
            collective_id=cid, has_side_effects=True, vmem_limit_bytes=56 * 1024 * 1024
        ),
    )(x, gain, w_qkv, w_out, mask)


def on_device(n, mp, grid, g2m_weight, g2m_slot, slot_node, peer_mask, norm_gain, w_qkv, w_out):
    cap = slot_node.shape[2]
    slots = n * cap
    scaled = (g2m_weight[:, None] * grid.astype(jnp.float32)).astype(jnp.bfloat16)
    slot_hot = (g2m_slot[None, :] == jnp.arange(slots, dtype=jnp.int32)[:, None]).astype(
        jnp.bfloat16
    )
    partial_value = jnp.dot(slot_hot, scaled, preferred_element_type=jnp.float32).astype(
        jnp.bfloat16
    )
    mesh_in = exchange(partial_value, n, 0)
    seen = [jnp.ones((1,), jnp.float32)]
    for column in MASK_COLUMN:
        seen.append(peer_mask[0, column : column + 1].astype(jnp.float32))
    mask = jnp.broadcast_to(jnp.concatenate(seen)[:, None, None], (len(OFFSETS), 1, slots))
    state, back = layer(mesh_in, norm_gain[None, :], w_qkv, w_out, mask, n, mp, 1)
    returned = exchange(back, n, 2)
    flat_nodes = slot_node[0].reshape(-1)
    node_hot = (jnp.arange(slots, dtype=jnp.int32)[:, None] == flat_nodes[None, :]).astype(
        jnp.bfloat16
    )
    low = (state - back.astype(jnp.float32)).astype(jnp.bfloat16)
    mesh_state = jnp.dot(node_hot, back, preferred_element_type=jnp.float32) + jnp.dot(
        node_hot, low, preferred_element_type=jnp.float32
    )
    gathered = jnp.dot(slot_hot.T, returned, preferred_element_type=jnp.float32)
    grid_out = (grid.astype(jnp.float32) + gathered).astype(jnp.bfloat16)
    return (mesh_state, grid_out)


def solution(mesh):
    return jax.shard_map(
        functools.partial(on_device, mesh.shape["region"], mesh.shape["mp"]),
        mesh=mesh,
        in_specs=(
            P("region", "mp"),
            P("region"),
            P("region"),
            P("region", None, None),
            P("region", None),
            P(),
            P(None, None, "mp"),
            P("mp", None),
        ),
        out_specs=(P("region", "mp"), P("region", "mp")),
        check_vma=False,
    )
```

```python
import functools

import jax
import jax.numpy as jnp
from jax import lax
from jax.experimental import pallas as pl
from jax.experimental.pallas import tpu as pltpu
from jax.sharding import PartitionSpec as P

HEAD_DIM = 64
PAD = 80
PEERS = 4
NEAR, RELAYED = 1, 2
MESH = pl.DeviceIdType.MESH
LOG2E = 1.4426950408889634


def exchange_kernel(n, meanwhile, x_ref, *refs):
    *extra, send, recv, local = refs
    o_ref = extra[-1] if meanwhile is None else extra[-2]
    me = lax.axis_index("region")
    rows = x_ref.shape[0] // n
    barrier = pltpu.get_barrier_semaphore()

    def hello(d, carry):
        pl.semaphore_signal(
            barrier, inc=1, device_id={"region": lax.rem(me + d, n)}, device_id_type=MESH
        )
        return carry

    lax.fori_loop(1, n, hello, 0)
    mine = pl.ds(pl.multiple_of(me * rows, rows), rows)
    own = pltpu.make_async_copy(x_ref.at[mine], o_ref.at[mine], local)
    own.start()
    pl.semaphore_wait(barrier, n - 1)

    def copy(d):
        peer = lax.rem(me + d, n)
        return pltpu.make_async_remote_copy(
            src_ref=x_ref.at[pl.ds(pl.multiple_of(peer * rows, rows), rows)],
            dst_ref=o_ref.at[mine],
            send_sem=send.at[d],
            recv_sem=recv.at[d],
            device_id={"region": peer},
            device_id_type=MESH,
        )

    def begin(d, carry):
        copy(d).start()
        return carry

    def finish(d, carry):
        copy(d).wait()
        return carry

    lax.fori_loop(1, n, begin, 0)
    if meanwhile is not None:
        meanwhile(x_ref, *extra)
    own.wait()
    lax.fori_loop(1, n, finish, 0)


def to_node_order(back_ref, state_ref, hot_ref, _, out_ref):
    low = (state_ref[...] - back_ref[...].astype(jnp.float32)).astype(jnp.bfloat16)
    out_ref[...] = jnp.dot(
        hot_ref[...], back_ref[...], preferred_element_type=jnp.float32
    ) + jnp.dot(hot_ref[...], low, preferred_element_type=jnp.float32)


def exchange(x, n, cid, meanwhile=None, extra_in=(), extra_out=()):
    vmem = pl.BlockSpec(memory_space=pltpu.VMEM)
    return pl.pallas_call(
        functools.partial(exchange_kernel, n, meanwhile),
        out_shape=(jax.ShapeDtypeStruct(x.shape, x.dtype),) + extra_out,
        in_specs=[vmem] * (1 + len(extra_in)),
        out_specs=(vmem,) * (1 + len(extra_out)),
        scratch_shapes=[
            pltpu.SemaphoreType.DMA((n,)),
            pltpu.SemaphoreType.DMA((n,)),
            pltpu.SemaphoreType.DMA,
        ],
        compiler_params=pltpu.CompilerParams(collective_id=cid, has_side_effects=True),
    )(x, *extra_in)


def layer_kernel(
    n, mp, x_ref, gain_ref, w_ref, wo_ref, row_ref, column_ref, state_ref, back_ref,
    gath, nrm, qm, kown, kbuf, vbuf, acc, top, att, out_part, in_part,
    local, psend, precv, msend, mrecv, rsend, rrecv,
):
    region = lax.axis_index("region")
    core = lax.axis_index("mp")
    rows, width = x_ref.shape
    heads = width // HEAD_DIM
    peers = PEERS
    chunk = rows // peers
    blocks = 1 + peers
    barrier = pltpu.get_barrier_semaphore()
    odd = lax.rem(region, 2)
    partner = region + 1 - 2 * odd
    below, above = lax.rem(region - 2 + n, n), lax.rem(region + 2, n)
    far = (peers - 1) * (1 - odd)
    for other in (below, partner, above):
        pl.semaphore_signal(barrier, inc=1, device_id={"region": other}, device_id_type=MESH)
    for j in range(1, mp):
        pl.semaphore_signal(
            barrier, inc=1, device_id={"mp": lax.rem(core + j, mp)}, device_id_type=MESH
        )
    own = pltpu.make_async_copy(x_ref, gath.at[0, core], local)
    own.start()
    acc[...] = jnp.zeros_like(acc)
    top[...] = jnp.full_like(top, -1e30)
    pl.semaphore_wait(barrier, 3 + mp - 1)

    def to_core(s, j):
        return pltpu.make_async_remote_copy(
            src_ref=x_ref if isinstance(s, int) else gath.at[s, core],
            dst_ref=gath.at[s, core],
            send_sem=msend.at[s, j],
            recv_sem=mrecv.at[s, j],
            device_id={"mp": lax.rem(core + j, mp)},
            device_id_type=MESH,
        )

    def to_peer(place, c, other):
        return pltpu.make_async_remote_copy(
            src_ref=x_ref.at[pl.ds(pl.multiple_of(c * chunk, chunk), chunk)],
            dst_ref=gath.at[1 + c, core, pl.ds(place * chunk, chunk)],
            send_sem=psend.at[c, place],
            recv_sem=precv.at[c, place],
            device_id={"region": other},
            device_id_type=MESH,
        )

    direct = ((0, above), (peers - 1, below), (NEAR, partner))

    def to_partner(c):
        return pltpu.make_async_remote_copy(
            src_ref=gath.at[1 + c, core, pl.ds(pl.multiple_of(far * chunk, chunk), chunk)],
            dst_ref=gath.at[1 + c, core, pl.ds(RELAYED * chunk, chunk)],
            send_sem=psend.at[c, RELAYED],
            recv_sem=precv.at[c, RELAYED],
            device_id={"region": partner},
            device_id_type=MESH,
        )

    def arrived(c, place):
        pltpu.make_async_remote_copy(
            src_ref=x_ref.at[pl.ds(0, chunk)],
            dst_ref=gath.at[1 + c, core, pl.ds(pl.multiple_of(place * chunk, chunk), chunk)],
            send_sem=psend.at[c, place],
            recv_sem=precv.at[c, place],
            device_id={"region": partner},
            device_id_type=MESH,
        ).wait_recv()

    for j in range(1, mp):
        to_core(0, j).start()
    for c in range(peers):
        for place, other in direct:
            to_peer(place, c, other).start()
    own.wait()

    def pass_on(s):
        arrived(s - 1, far)
        to_partner(s - 1).start()

    def relay(s):
        arrived(s - 1, peers - 1 - far)
        arrived(s - 1, NEAR)
        arrived(s - 1, RELAYED)
        for j in range(1, mp):
            to_core(s, j).start()

    def block(s, carry):
        for j in range(1, mp):
            to_core(s, j).wait_recv()
        square = jnp.zeros((rows, 1), jnp.float32)
        for m in range(mp):
            part = gath[s, m].astype(jnp.float32)
            square += jnp.sum(part * part, axis=-1, keepdims=True)
        inv = lax.rsqrt(square / (mp * width) + 1e-05)
        for m in range(mp):
            cols = slice(m * width, (m + 1) * width)
            nrm[:, cols] = (gath[s, m].astype(jnp.float32) * inv * gain_ref[:, cols]).astype(
                jnp.bfloat16
            )
        kind = jnp.minimum(s, 1)
        seen = row_ref[kind]

        @pl.when(s == 0)
        def _():
            q = jnp.dot(nrm[...], w_ref[0], preferred_element_type=jnp.float32)
            q = q * (LOG2E * HEAD_DIM ** (-0.5))
            lane = lax.broadcasted_iota(jnp.int32, (rows, 2 * HEAD_DIM), 1)
            for h in range(heads):
                pair = q[:, h // 2 * 2 * HEAD_DIM : (h // 2 + 1) * 2 * HEAD_DIM]
                keep = (lane < HEAD_DIM) if h % 2 == 0 else (lane >= HEAD_DIM)
                qm[h] = jnp.where(keep, pair, 0.0).astype(jnp.bfloat16)

        keys = jnp.dot(nrm[...], w_ref[1], preferred_element_type=jnp.float32)

        @pl.when(s == 0)
        def _():
            kown[...] = keys

        keys = jnp.where(column_ref[kind] > 0, keys, kown[...])
        for g in range(heads // 2):
            kbuf[g] = keys[:, g * 2 * HEAD_DIM : (g + 1) * 2 * HEAD_DIM].astype(jnp.bfloat16)
        vals = jnp.dot(nrm[...], w_ref[2], preferred_element_type=jnp.float32)
        turned = vals.T * seen
        row = lax.broadcasted_iota(jnp.int32, (PAD - HEAD_DIM, rows), 0)
        extra = jnp.where(row == 0, jnp.broadcast_to(seen, row.shape), 0.0).astype(jnp.bfloat16)
        for h in range(heads):
            vbuf[h, :HEAD_DIM] = turned[h * HEAD_DIM : (h + 1) * HEAD_DIM].astype(jnp.bfloat16)
            vbuf[h, HEAD_DIM:] = extra

        @pl.when(jnp.logical_and(s >= 1, s < blocks - 1))
        def _():
            relay(s + 1)

        def two_heads(g, carry):
            key = kbuf[g]
            for e in range(2):
                h = 2 * g + e
                scores = lax.dot_general(
                    key, qm[h], (((1,), (1,)), ((), ())), preferred_element_type=jnp.float32
                )
                old = top[h]
                new = jnp.maximum(old, jnp.max(scores, axis=0, keepdims=True))
                weights = jnp.exp2(scores - new).astype(jnp.bfloat16)
                acc[h] = acc[h] * jnp.exp2(old - new) + jnp.dot(
                    vbuf[h], weights, preferred_element_type=jnp.float32
                )
                top[h] = new
            return carry

        lax.fori_loop(0, heads // 4, two_heads, 0)

        @pl.when(s == 0)
        def _():
            pass_on(s + 1)

        @pl.when(jnp.logical_and(s >= 1, s < blocks - 2))
        def _():
            pass_on(s + 2)

        lax.fori_loop(heads // 4, heads // 2, two_heads, 0)

        @pl.when(s == 0)
        def _():
            relay(s + 1)
            pass_on(s + 2)

        return carry

    lax.fori_loop(0, blocks, block, 0)
    for h in range(heads):
        mix = acc[h]
        att[h * HEAD_DIM : (h + 1) * HEAD_DIM] = mix[:HEAD_DIM] / mix[HEAD_DIM : HEAD_DIM + 1]
    attended = att[...].T.astype(jnp.bfloat16)

    def product(m):
        cols = pl.ds(pl.multiple_of(m * width, width), width)
        return jnp.dot(attended, wo_ref[:, cols], preferred_element_type=jnp.float32)

    def share(j):
        return pltpu.make_async_remote_copy(
            src_ref=out_part.at[j],
            dst_ref=in_part.at[j],
            send_sem=rsend.at[j],
            recv_sem=rrecv.at[j],
            device_id={"mp": lax.rem(core + j, mp)},
            device_id_type=MESH,
        )

    for j in range(1, mp):
        out_part[j] = product(lax.rem(core + j, mp))
        share(j).start()
    total = x_ref[...].astype(jnp.float32) + product(core)
    for j in range(1, mp):
        share(j).wait()
        total += in_part[j]
    state_ref[...] = total
    back_ref[...] = total.astype(jnp.bfloat16)
    for c in range(peers):
        for place, other in direct:
            to_peer(place, c, other).wait_send()
        to_partner(c).wait_send()

    def drain(s, carry):
        for j in range(1, mp):
            to_core(s, j).wait_send()
        return carry

    lax.fori_loop(0, blocks, drain, 0)


def layer(x, gain, w_qkv, w_out, row_mask, column_mask, n, mp, cid):
    rows, width = x.shape
    heads = width // HEAD_DIM
    peers = PEERS
    blocks = 1 + peers
    bf16, f32 = jnp.bfloat16, jnp.float32
    vmem = pl.BlockSpec(memory_space=pltpu.VMEM)
    dma = pltpu.SemaphoreType.DMA
    return pl.pallas_call(
        functools.partial(layer_kernel, n, mp),
        out_shape=(
            jax.ShapeDtypeStruct((rows, width), f32),
            jax.ShapeDtypeStruct((rows, width), bf16),
        ),
        in_specs=[vmem] * 6,
        out_specs=(vmem, vmem),
        scratch_shapes=[
            pltpu.VMEM((blocks, mp, rows, width), bf16),
            pltpu.VMEM((rows, mp * width), bf16),
            pltpu.VMEM((heads, rows, 2 * HEAD_DIM), bf16),
            pltpu.VMEM((rows, width), f32),
            pltpu.VMEM((heads // 2, rows, 2 * HEAD_DIM), bf16),
            pltpu.VMEM((heads, PAD, rows), bf16),
            pltpu.VMEM((heads, PAD, rows), f32),
            pltpu.VMEM((heads, 1, rows), f32),
            pltpu.VMEM((width, rows), f32),
            pltpu.VMEM((mp, rows, width), f32),
            pltpu.VMEM((mp, rows, width), f32),
            dma,
            dma((peers, peers)),
            dma((peers, peers)),
            dma((blocks, mp)),
            dma((blocks, mp)),
            dma((mp,)),
            dma((mp,)),
        ],
        compiler_params=pltpu.CompilerParams(
            collective_id=cid, has_side_effects=True, vmem_limit_bytes=56 * 1024 * 1024
        ),
    )(x, gain, w_qkv, w_out, row_mask, column_mask)


def on_device(n, mp, grid, g2m_weight, g2m_slot, slot_node, peer_mask, norm_gain, w_qkv, w_out):
    cap = slot_node.shape[2]
    slots = n * cap
    scaled = (g2m_weight[:, None] * grid.astype(jnp.float32)).astype(jnp.bfloat16)
    slot_hot = (g2m_slot[None, :] == jnp.arange(slots, dtype=jnp.int32)[:, None]).astype(
        jnp.bfloat16
    )
    partial_value = jnp.dot(slot_hot, scaled, preferred_element_type=jnp.float32).astype(
        jnp.bfloat16
    )
    (mesh_in,) = exchange(partial_value, n, 0)
    two_below, below, above, two_above = (peer_mask[0, c : c + 1] for c in range(PEERS))
    odd = lax.axis_index("region") % 2 == 1
    places = jnp.concatenate(
        [two_below, jnp.where(odd, below, above), jnp.where(odd, above, below), two_above]
    )
    peer_seen = jnp.repeat(places.astype(jnp.float32), slots // PEERS)
    seen = jnp.stack([jnp.ones_like(peer_seen), peer_seen])
    state, back = layer(
        mesh_in, norm_gain[None, :], w_qkv, w_out, seen[:, None, :], seen[:, :, None], n, mp, 1
    )
    flat_nodes = slot_node[0].reshape(-1)
    node_hot = (jnp.arange(slots, dtype=jnp.int32)[:, None] == flat_nodes[None, :]).astype(
        jnp.bfloat16
    )
    returned, mesh_state = exchange(
        back,
        n,
        2,
        to_node_order,
        (state, node_hot),
        (jax.ShapeDtypeStruct(state.shape, state.dtype),),
    )
    gathered = jnp.dot(slot_hot.T, returned, preferred_element_type=jnp.float32)
    grid_out = (grid.astype(jnp.float32) + gathered).astype(jnp.bfloat16)
    return (mesh_state, grid_out)


def solution(mesh):
    return jax.shard_map(
        functools.partial(on_device, mesh.shape["region"], mesh.shape["mp"]),
        mesh=mesh,
        in_specs=(
            P("region", "mp"),
            P("region"),
            P("region"),
            P("region", None, None),
            P("region", None),
            P(),
            P(None, None, "mp"),
            P("mp", None),
        ),
        out_specs=(P("region", "mp"), P("region", "mp")),
        check_vma=False,
    )
```
